128 devices in a mesh: ya: 32 (over z, y, core), zb: 4 (over x).
Axes of the slice: x: 4, y: 4, z: 4, core: 2. Of those that a mesh axis runs over, the one named last changes fastest.
Arguments:
- source: float32 [512, 512, 512], P(None, 'ya', 'zb'), may hold values from -6 to 6
- symbol_x: float32 [512], replicated, may hold values from 0.3 to 3
- symbol_y: float32 [512], replicated, may hold values from 0.3 to 3
- symbol_z: float32 [512], replicated, may hold values from 0.3 to 3
Outputs:
- modes: float32 [512, 512, 512], P('ya', 'zb')
The draws below stay inside these ranges and needn't reach their ends.
All inputs are finite; a program needn't handle non-finite values.
Results may differ from the reference program's by a relative error of at most 0.000071.
Values sent between devices are 32-bit elements; how exact they have to be, the bound alone decides.
A program may use at most 64 MiB of HBM per device.

```python
import jax
import jax.numpy as jnp
from jax import lax

GRID_X = 512
GRID_Y = 512
GRID_Z = 512


def block_levels(rng, shape, shards, low, top_value):
    def one(dim, parts):
        heights = jax.random.uniform(jax.random.fold_in(jax.random.fold_in(rng, 6), dim), (parts,), jnp.float32, low / len(shards), top_value / len(shards))
        return jnp.repeat(jnp.exp(heights), shape[dim] // parts).reshape((-1,) + (1,) * (len(shape) - dim - 1))

    gain = one(*shards[0])
    for cut in shards[1:]:
        gain = gain * one(*cut)
    return gain


def noise(rng, shape, width, limit, split=(), dtype=jnp.bfloat16):
    drawn = width * jax.random.normal(rng, shape, jnp.float32)
    if split:
        drawn = drawn * block_levels(rng, shape, split, -0.22, 0.18)
    return jnp.clip(drawn, -limit, limit).astype(dtype)


def setup_inputs(seed: int = 0) -> dict:
    splits = jax.random.split(jax.random.key(seed), 5)
    source = noise(splits[0], (GRID_X, GRID_Y, GRID_Z), 1.0, 6.0, ((1, 32), (2, 4)), jnp.float32)
    symbol_x = jnp.clip(jax.random.uniform(splits[1], (GRID_X,), jnp.float32, 0.3, 3.0), 0.3, 3.0)
    symbol_y = jnp.clip(jax.random.uniform(splits[2], (GRID_Y,), jnp.float32, 0.3, 3.0), 0.3, 3.0)
    symbol_z = jnp.clip(jax.random.uniform(splits[3], (GRID_Z,), jnp.float32, 0.3, 3.0), 0.3, 3.0)
    return {"source": source, "symbol_x": symbol_x, "symbol_y": symbol_y, "symbol_z": symbol_z}


def transform_table(count):
    rank = jnp.arange(count)
    angle = jnp.pi / (count + 1) * ((rank[:, None] + 1) * (rank[None, :] + 1) % (2 * count + 2)).astype(jnp.float32)
    return jnp.sin(angle) * (2.0 / (count + 1)) ** 0.5

def transform_dim(values, dim):
    moved = jnp.tensordot(values, transform_table(values.shape[dim]), axes=([dim], [0]), precision=lax.Precision.HIGHEST)
    return jnp.moveaxis(moved, -1, dim)

def reference(source, symbol_x, symbol_y, symbol_z):
    modes = source
    modes = transform_dim(modes, 0)
    modes = transform_dim(modes, 1)
    modes = transform_dim(modes, 2)
    symbol = symbol_x[:, None, None] + symbol_y[None, :, None] + symbol_z[None, None, :]
    modes = modes * lax.rsqrt(symbol)
    return modes
```

```python
import functools

import jax
import jax.numpy as jnp
import ml_dtypes
import numpy as np
from jax import lax
from jax.experimental import pallas as pl
from jax.experimental.pallas import tpu as pltpu
from jax.sharding import PartitionSpec as P

MESH = pl.DeviceIdType.MESH
N = 512
CHUNKS = (2, 2, 2, 2, 2, 2, 2, 2)
STEP = 7


def table():
    rank = np.arange(1, N + 1)
    angle = np.pi * (rank[:, None] * rank[None, :] % (2 * N + 2)) / (N + 1)
    return np.sqrt(2.0 / (N + 1)) * np.sin(angle)


def halves(h):
    high = h.astype(ml_dtypes.bfloat16)
    return high, (h - high.astype(np.float64)).astype(ml_dtypes.bfloat16)


def split(v):
    high = v.astype(jnp.bfloat16)
    return high, (v - high.astype(jnp.float32)).astype(jnp.bfloat16)


def dot3(ah, al, bh, bl):
    d = functools.partial(jnp.dot, preferred_element_type=jnp.float32)
    return d(ah, bh) + (d(al, bh) + d(ah, bl))


def kernel(
    src, h1h_hbm, h1l_hbm, hh_hbm, hl_hbm, sx, sy, sz, out,
    xin, xh, xl, h1h, h1l, hh, hl, a_out, a_in, b_out, b_in, ycol,
    load_sem, table_sem, a_send, a_recv, a_own, b_send, b_recv,
):
    ya, zb = lax.axis_index("ya"), lax.axis_index("zb")
    tables = [
        pltpu.make_async_copy(s, d, table_sem.at[k])
        for k, (s, d) in enumerate(((h1h_hbm, h1h), (h1l_hbm, h1l), (hh_hbm, hh), (hl_hbm, hl)))
    ]
    load = pltpu.make_async_copy(src, xin, load_sem)
    load.start()
    for t in tables:
        t.start()

    def peer_a(i):
        o = lax.rem(i * STEP, 31) + 1
        core = lax.rem(ya + o, 2)
        y = lax.rem(ya // 2 + o // 2, 4)
        z = lax.rem(ya // 8 + o // 8, 4)
        return z * 8 + y * 2 + core

    barrier = pltpu.get_barrier_semaphore()

    @pl.loop(0, 31)
    def _(i):
        pl.semaphore_signal(barrier, inc=1, device_id=(peer_a(i), zb), device_id_type=MESH)

    for d in (1, 3, 2):
        pl.semaphore_signal(barrier, inc=1, device_id=(ya, lax.rem(zb + d, 4)), device_id_type=MESH)

    ycol[...] = jnp.transpose(jnp.broadcast_to(sy[pl.ds(zb, 1), :], (128, 128)))
    load.wait()

    @pl.loop(0, 16)
    def _(y):
        high, low = split(xin[pl.ds(y, N, stride=16), :])
        xh[y] = high
        xl[y] = low

    tables[0].wait()
    tables[1].wait()

    starts = [sum(CHUNKS[:c]) for c in range(len(CHUNKS))]

    def transform_x(c):
        m0, mc = starts[c], CHUNKS[c]
        rows = 32 * mc

        @pl.loop(0, 8)
        def _(g):
            bh = jnp.concatenate([xh[2 * g], xh[2 * g + 1]], axis=1)
            bl = jnp.concatenate([xl[2 * g], xl[2 * g + 1]], axis=1)
            r = dot3(h1h[pl.ds(m0 * 32, rows), :], h1l[pl.ds(m0 * 32, rows), :], bh, bl)
            for k in range(2):
                a_out[pl.ds(m0 * 512 + 2 * g + k, rows, stride=16), :] = r[:, 128 * k : 128 * k + 128]

    def a_rows(c, who):
        m0, mc = starts[c], CHUNKS[c]
        return pl.ds(pl.multiple_of(m0 * 512 + who * (mc * 16), 16), mc * 16)

    def own_copy(c):
        return pltpu.make_async_copy(a_out.at[a_rows(c, ya)], a_in.at[a_rows(c, ya)], a_own.at[c])

    def send_a(c):
        own_copy(c).start()

        @pl.loop(0, 31)
        def _(i):
            peer = peer_a(i)
            pltpu.make_async_remote_copy(
                src_ref=a_out.at[a_rows(c, peer)],
                dst_ref=a_in.at[a_rows(c, ya)],
                send_sem=a_send.at[c],
                recv_sem=a_recv.at[c],
                device_id=(peer, zb),
                device_id_type=MESH,
            ).start()

    def a_all(ref, c):
        return ref.at[pl.ds(starts[c] * 512, 31 * CHUNKS[c] * 16)]

    def wait_a(c):
        own_copy(c).wait()
        pltpu.make_async_copy(a_all(a_in, c), a_all(a_in, c), a_recv.at[c]).wait()

    def b_blocks(c, who):
        m0, mc = starts[c], CHUNKS[c]
        return pl.ds(m0 * 4 + who * mc, mc)

    def transform_y(c):
        m0, mc = starts[c], CHUNKS[c]
        pairs = [(m, min(2, mc - m)) for m in range(0, mc, 2)]
        for m, count in pairs:
            v = jnp.concatenate(
                [
                    jnp.concatenate(
                        [a_in[pl.ds(m0 * 512 + (a * mc + m + k) * 16, 16), :] for a in range(32)], axis=0
                    )
                    for k in range(count)
                ],
                axis=1,
            )
            bh, bl = split(v)
            for d in (1, 3, 2, 0):
                b = lax.rem(zb + d, 4)
                rows = pl.ds(pl.multiple_of(b * 128, 128), 128)
                r = dot3(hh[rows, :], hl[rows, :], bh, bl)
                for k in range(count):
                    target = b_in if d == 0 else b_out
                    target[m0 * 4 + b * mc + m + k] = r[:, 128 * k : 128 * k + 128]
                if d and m + count == mc:
                    pltpu.make_async_remote_copy(
                        src_ref=b_out.at[b_blocks(c, b)],
                        dst_ref=b_in.at[b_blocks(c, zb)],
                        send_sem=b_send.at[c],
                        recv_sem=b_recv.at[c],
                        device_id=(ya, b),
                        device_id_type=MESH,
                    ).start()

    def b_all(ref, c):
        return ref.at[pl.ds(starts[c] * 4, 3 * CHUNKS[c])]

    def wait_b(c):
        pltpu.make_async_copy(b_all(b_in, c), b_all(b_in, c), b_recv.at[c]).wait()

    def transform_z(c):
        m0, mc = starts[c], CHUNKS[c]

        @pl.loop(0, mc)
        def _(m):
            v = jnp.concatenate([b_in[m0 * 4 + b * mc + m] for b in range(4)], axis=1)
            ah, al = split(v)
            r = dot3(ah, al, hh[...], hl[...])
            column = ycol[...] + sx[ya * 16 + m0 + m]
            for k in range(4):
                scale = lax.rsqrt(column + sz[pl.ds(k, 1), :])
                out[m0 + m, :, 128 * k : 128 * k + 128] = r[:, 128 * k : 128 * k + 128] * scale

    transform_x(0)
    pl.semaphore_wait(barrier, 34)
    send_a(0)
    transform_x(1)
    send_a(1)
    tables[2].wait()
    tables[3].wait()
    count = len(CHUNKS)
    for c in range(count):
        if c + 2 < count:
            transform_x(c + 2)
            send_a(c + 2)
        wait_a(c)
        transform_y(c)
        if c >= 1:
            wait_b(c - 1)
            transform_z(c - 1)
    wait_b(count - 1)
    transform_z(count - 1)
    for c in range(count):
        pltpu.make_async_copy(a_all(a_out, c), a_all(a_out, c), a_send.at[c]).wait()
        pltpu.make_async_copy(b_all(b_out, c), b_all(b_out, c), b_send.at[c]).wait()


def body(source, symbol_x, symbol_y, symbol_z):
    h = table()
    order = [a * 16 + m0 + m for m0, mc in zip(np.cumsum((0,) + CHUNKS[:-1]), CHUNKS) for a in range(32) for m in range(mc)]
    tables = [jnp.asarray(v) for v in halves(h[np.array(order)]) + halves(h)]
    any_space = pl.BlockSpec(memory_space=pl.ANY)
    vmem = pl.BlockSpec(memory_space=pltpu.VMEM)
    smem = pl.BlockSpec(memory_space=pltpu.SMEM)
    f32, bf16, count = jnp.float32, jnp.bfloat16, len(CHUNKS)
    return pl.pallas_call(
        kernel,
        out_shape=jax.ShapeDtypeStruct((16, 128, 512), f32),
        in_specs=[any_space] * 5 + [smem, vmem, vmem],
        out_specs=vmem,
        scratch_shapes=[
            pltpu.VMEM((512 * 16, 128), f32),
            pltpu.VMEM((16, 512, 128), bf16),
            pltpu.VMEM((16, 512, 128), bf16),
            pltpu.VMEM((512, 512), bf16),
            pltpu.VMEM((512, 512), bf16),
            pltpu.VMEM((512, 512), bf16),
            pltpu.VMEM((512, 512), bf16),
            pltpu.VMEM((8192, 128), f32),
            pltpu.VMEM((8192, 128), f32),
            pltpu.VMEM((64, 128, 128), f32),
            pltpu.VMEM((64, 128, 128), f32),
            pltpu.VMEM((128, 128), f32),
            pltpu.SemaphoreType.DMA,
            pltpu.SemaphoreType.DMA((4,)),
            pltpu.SemaphoreType.DMA((count,)),
            pltpu.SemaphoreType.DMA((count,)),
            pltpu.SemaphoreType.DMA((count,)),
            pltpu.SemaphoreType.DMA((count,)),
            pltpu.SemaphoreType.DMA((count,)),
        ],
        compiler_params=pltpu.CompilerParams(
            collective_id=0, has_side_effects=True, vmem_limit_bytes=48 * 1024 * 1024
        ),
    )(source.reshape(8192, 128), *tables, symbol_x, symbol_y.reshape(4, 128), symbol_z.reshape(4, 128))


def solution(mesh):
    placed = (P(None, "ya", "zb"), P(), P(), P())
    return jax.shard_map(
        body, mesh=mesh, in_specs=placed, out_specs=P("ya", "zb", None), check_vma=False
    )
```

```python
import functools

import jax
import jax.numpy as jnp
import ml_dtypes
import numpy as np
from jax import lax
from jax.experimental import pallas as pl
from jax.experimental.pallas import tpu as pltpu
from jax.sharding import PartitionSpec as P

MESH = pl.DeviceIdType.MESH


def scoped(f):
    def g(*args):
        with jax.named_scope(f.__name__):
            return f(*args)

    return g

N = 512
ORDER = [i * 7 % 31 + 1 for i in range(31)]
EARLY = 2
YPARTS = ((1, 3), (2, 0))
AHEAD = 5
LAG = 2


def table():
    rank = np.arange(1, N + 1)
    angle = np.pi * (rank[:, None] * rank[None, :] % (2 * N + 2)) / (N + 1)
    return np.sqrt(2.0 / (N + 1)) * np.sin(angle)


def halves(h):
    high = h.astype(ml_dtypes.bfloat16)
    return high, (h - high.astype(np.float64)).astype(ml_dtypes.bfloat16)


def split(v):
    high = v.astype(jnp.bfloat16)
    return high, (v - high.astype(jnp.float32)).astype(jnp.bfloat16)


def dot(a, b):
    return jnp.dot(a, b, preferred_element_type=jnp.float32)


def kernel(
    src, h1_hbm, hh_hbm, hl_hbm, sx_hbm, sy_hbm, sz_hbm, out,
    xin, xh, xl, h1, hh, hl, a_early, a_out, a_in, b_out, b_in, ycol, sx, sy, sz,
    load_sem, table_sem, a_send, a_recv, a_own, b_send, b_recv,
):
    ya, zb = lax.axis_index("ya"), lax.axis_index("zb")

    def load(y):
        return pltpu.make_async_copy(src.at[:, y, 0, :], xin.at[y], load_sem.at[y])

    tables = [
        pltpu.make_async_copy(s, d, table_sem.at[k])
        for k, (s, d) in enumerate(
            ((h1_hbm, h1), (hh_hbm, hh), (hl_hbm, hl), (sx_hbm, sx), (sy_hbm, sy), (sz_hbm, sz))
        )
    ]
    tables[0].start()
    for y in range(16):
        load(y).start()

    def peer_a(o):
        return ya ^ o

    barrier = pltpu.get_barrier_semaphore()
    for o in ORDER:
        pl.semaphore_signal(barrier, inc=1, device_id=(peer_a(o), zb), device_id_type=MESH)
    for d in (1, 3, 2):
        pl.semaphore_signal(barrier, inc=1, device_id=(ya, (zb + d) & 3), device_id_type=MESH)
    for t in tables[1:]:
        t.start()

    def a_slot(c, who):
        return a_in.at[pl.ds(pl.multiple_of(c * 512 + who * 16, 16), 16)]

    def a_source(c, who):
        if isinstance(c, int) and c < EARLY:
            return a_early.at[pl.ds(pl.multiple_of(c * 512 + who * 16, 16), 16)]
        return a_out.at[pl.ds(pl.multiple_of(who * 256 + c * 16, 16), 16)]

    def a_all(c):
        return a_in.at[pl.ds(pl.multiple_of(c * 512, 512), 31 * 16)]

    @scoped
    def send_a(c):
        pltpu.make_async_copy(a_source(c, ya), a_slot(c, ya), a_own.at[c]).start()
        for o in ORDER:
            peer = peer_a(o)
            pltpu.make_async_remote_copy(
                src_ref=a_source(c, peer),
                dst_ref=a_slot(c, ya),
                send_sem=a_send.at[c],
                recv_sem=a_recv.at[c],
                device_id=(peer, zb),
                device_id_type=MESH,
            ).start()

    @scoped
    def wait_a(c):
        pltpu.make_async_copy(a_slot(c, ya), a_slot(c, ya), a_own.at[c]).wait()
        pltpu.make_async_copy(a_all(c), a_all(c), a_recv.at[c]).wait()

    @scoped
    def transform_y(c):
        bh, bl = split(a_in[pl.ds(pl.multiple_of(c * 512, 512), 512), :])
        rhs = jnp.concatenate([bh, bh, bl], axis=0)
        for ds in YPARTS:
            blocks = [(zb + d) & 3 for d in ds]
            rows = [pl.ds(pl.multiple_of(b * 128, 128), 128) for b in blocks]
            high = jnp.concatenate([hh[r, :] for r in rows], axis=0)
            low = jnp.concatenate([hl[r, :] for r in rows], axis=0)
            r = dot(jnp.concatenate([high, low, high], axis=1), rhs)
            for i, (d, b) in enumerate(zip(ds, blocks)):
                target = b_out if d else b_in
                target[c * 4 + b] = r[128 * i : 128 * i + 128, :]
                if d:
                    pltpu.make_async_remote_copy(
                        src_ref=b_out.at[c * 4 + b],
                        dst_ref=b_in.at[c * 4 + zb],
                        send_sem=b_send.at[c],
                        recv_sem=b_recv.at[c],
                        device_id=(ya, b),
                        device_id_type=MESH,
                    ).start()

    def b_all(ref, c):
        return ref.at[pl.ds(c * 4, 3)]

    @scoped
    def wait_b(c):
        pltpu.make_async_copy(b_all(b_in, c), b_all(b_in, c), b_recv.at[c]).wait()

    @scoped
    def transform_z(c):
        ah, al = split(jnp.concatenate([b_in[c * 4 + b] for b in range(4)], axis=1))
        lhs = jnp.concatenate([ah, ah, al], axis=1)
        column = ycol[...] + sx[ya * 16 + c]
        for k in range(2):
            cols = slice(256 * k, 256 * k + 256)
            rhs = jnp.concatenate([hh[:, cols], hl[:, cols], hh[:, cols]], axis=0)
            r = dot(lhs, rhs)
            for j in range(2):
                n = 2 * k + j
                scale = lax.rsqrt(column + sz[pl.ds(n, 1), :])
                out[c, :, 128 * n : 128 * n + 128] = r[:, 128 * j : 128 * j + 128] * scale

    rows = 32 * EARLY
    with jax.named_scope("early"):
        for g in range(4):
            bhs, bls = [], []
            for y in range(4 * g, 4 * g + 4):
                load(y).wait()
                high, low = split(xin[y])
                xh[y] = high
                xl[y] = low
                bhs.append(high)
                bls.append(low)
            if g == 0:
                tables[0].wait()
            bh, bl = jnp.concatenate(bhs, axis=1), jnp.concatenate(bls, axis=1)
            both = dot(h1[...], bh)
            r = both[:rows] + (both[rows:] + dot(h1[pl.ds(0, rows), :], bl))
            for k in range(4):
                a_early[pl.ds(4 * g + k, rows, stride=16), :] = r[:, 128 * k : 128 * k + 128]
    with jax.named_scope("barrier_wait"):
        pl.semaphore_wait(barrier, 34)
    for c in range(EARLY):
        send_a(c)
    for t in tables[1:]:
        t.wait()
    with jax.named_scope("rest"):

        @pl.loop(0, 8)
        def _(g):
            bh = jnp.concatenate([xh[2 * g], xh[2 * g + 1]], axis=1)
            bl = jnp.concatenate([xl[2 * g], xl[2 * g + 1]], axis=1)
            rhs = jnp.concatenate([bh, bh, bl], axis=0)
            r = dot(jnp.concatenate([hh[...], hl[...], hh[...]], axis=1), rhs)
            for k in range(2):
                a_out[pl.ds(2 * g + k, 512, stride=16), :] = r[:, 128 * k : 128 * k + 128]

    @pl.loop(EARLY, AHEAD)
    def _(c):
        send_a(c)

    ycol[...] = jnp.transpose(jnp.broadcast_to(sy[pl.ds(zb, 1), :], (128, 128)))

    @pl.loop(0, 16)
    def _(c):
        wait_a(c)
        transform_y(c)

        @pl.when(c + AHEAD < 16)
        def _():
            send_a(c + AHEAD)

        @pl.when(c >= LAG)
        def _():
            wait_b(c - LAG)
            transform_z(c - LAG)

    @pl.loop(16 - LAG, 16)
    def _(c):
        wait_b(c)
        transform_z(c)

    with jax.named_scope("drain"):

        @pl.loop(0, 16)
        def _(c):
            pltpu.make_async_copy(a_all(c), a_all(c), a_send.at[c]).wait()
            pltpu.make_async_copy(b_all(b_out, c), b_all(b_out, c), b_send.at[c]).wait()


def body(source, symbol_x, symbol_y, symbol_z):
    high, low = halves(table())
    order = np.array([a * 16 + c for c in range(EARLY) for a in range(32)])
    stacked = np.concatenate([high[order], low[order]])
    any_space = pl.BlockSpec(memory_space=pl.ANY)
    f32, bf16 = jnp.float32, jnp.bfloat16
    return pl.pallas_call(
        kernel,
        out_shape=pltpu.VMEM((16, 128, 512), f32),
        in_specs=[any_space] * 7,
        out_specs=pl.BlockSpec(memory_space=pltpu.VMEM),
        scratch_shapes=[
            pltpu.VMEM((16, 512, 128), f32),
            pltpu.VMEM((16, 512, 128), bf16),
            pltpu.VMEM((16, 512, 128), bf16),
            pltpu.VMEM(stacked.shape, bf16),
            pltpu.VMEM((512, 512), bf16),
            pltpu.VMEM((512, 512), bf16),
            pltpu.VMEM((len(order) * 16, 128), f32),
            pltpu.VMEM((8192, 128), f32),
            pltpu.VMEM((8192, 128), f32),
            pltpu.VMEM((64, 128, 128), f32),
            pltpu.VMEM((64, 128, 128), f32),
            pltpu.VMEM((128, 128), f32),
            pltpu.SMEM((512,), f32),
            pltpu.VMEM((4, 128), f32),
            pltpu.VMEM((4, 128), f32),
            pltpu.SemaphoreType.DMA((16,)),
            pltpu.SemaphoreType.DMA((6,)),
            pltpu.SemaphoreType.DMA((16,)),
            pltpu.SemaphoreType.DMA((16,)),
            pltpu.SemaphoreType.DMA((16,)),
            pltpu.SemaphoreType.DMA((16,)),
            pltpu.SemaphoreType.DMA((16,)),
        ],
        compiler_params=pltpu.CompilerParams(
            collective_id=0, has_side_effects=True, vmem_limit_bytes=67043328 - 4 * 1024 * 1024 - 65536
        ),
    )(
        source.reshape(512, 16, 1, 128),
        jnp.asarray(stacked),
        jnp.asarray(high),
        jnp.asarray(low),
        symbol_x,
        symbol_y.reshape(4, 128),
        symbol_z.reshape(4, 128),
    )


def solution(mesh):
    placed = (P(None, "ya", "zb"), P(), P(), P())
    return jax.shard_map(
        body, mesh=mesh, in_specs=placed, out_specs=P("ya", "zb", None), check_vma=False
    )
```

```python
import functools

import jax
import jax.numpy as jnp
import ml_dtypes
import numpy as np
from jax import lax
from jax.experimental import pallas as pl
from jax.experimental.pallas import tpu as pltpu
from jax.sharding import PartitionSpec as P

MESH = pl.DeviceIdType.MESH


def scoped(f):
    def g(*args):
        with jax.named_scope(f.__name__):
            return f(*args)

    return g

N = 512
FAR = (10, 11, 14, 9, 6, 5, 7, 13, 15, 8, 2, 1, 4, 3, 12)
EARLY = 2
YPARTS = ((1, 3), (2, 0))
AHEAD = 3
LAG = 2


def table():
    rank = np.arange(1, N + 1)
    angle = np.pi * (rank[:, None] * rank[None, :] % (2 * N + 2)) / (N + 1)
    return np.sqrt(2.0 / (N + 1)) * np.sin(angle)


def halves(h):
    high = h.astype(ml_dtypes.bfloat16)
    return high, (h - high.astype(np.float64)).astype(ml_dtypes.bfloat16)


def split(v):
    high = v.astype(jnp.bfloat16)
    return high, (v - high.astype(jnp.float32)).astype(jnp.bfloat16)


def dot(a, b):
    return jnp.dot(a, b, preferred_element_type=jnp.float32)


def kernel(
    src, h1_hbm, hh_hbm, hl_hbm, sx_hbm, sy_hbm, sz_hbm, out,
    xin, xh, xl, h1, hh, hl, a_early, a_out, a_in, b_out, b_in, ycol, sx, sy, sz,
    load_sem, table_sem, a_send, a_recv, b_send, b_recv,
):
    ya, zb = lax.axis_index("ya"), lax.axis_index("zb")

    def load(y):
        return pltpu.make_async_copy(src.at[:, y, 0, :], xin.at[y], load_sem.at[y // 4])

    tables = [
        pltpu.make_async_copy(s, d, table_sem.at[k])
        for k, (s, d) in enumerate(
            ((h1_hbm, h1), (hh_hbm, hh), (hl_hbm, hl), (sx_hbm, sx), (sy_hbm, sy), (sz_hbm, sz))
        )
    ]
    tables[0].start()

    chip, core = ya >> 1, ya & 1
    peers = [(chip ^ p) * 2 + 1 for p in FAR] + [chip * 2 + 1 - core] + [(chip ^ p) * 2 for p in FAR]

    barrier = pltpu.get_barrier_semaphore()
    for peer in peers:
        pl.semaphore_signal(barrier, inc=1, device_id=(peer, zb), device_id_type=MESH)
    for d in (1, 3, 2):
        pl.semaphore_signal(barrier, inc=1, device_id=(ya, (zb + d) & 3), device_id_type=MESH)
    for y in range(16):
        load(y).start()
    for t in tables[1:]:
        t.start()

    def a_slot(c, who):
        return a_in.at[pl.ds(pl.multiple_of(c * 512 + who * 16, 16), 16)]

    def a_source(c, who):
        if isinstance(c, int) and c < EARLY:
            return a_early.at[pl.ds(pl.multiple_of(c * 512 + who * 16, 16), 16)]
        return a_out.at[pl.ds(pl.multiple_of(who * 256 + c * 16, 16), 16)]

    @scoped
    def send_a(c):
        pltpu.make_async_copy(a_source(c, ya), a_slot(c, ya), a_recv.at[c]).start()
        for peer in peers:
            pltpu.make_async_remote_copy(
                src_ref=a_source(c, peer),
                dst_ref=a_slot(c, ya),
                send_sem=a_send,
                recv_sem=a_recv.at[c],
                device_id=(peer, zb),
                device_id_type=MESH,
            ).start()

    @scoped
    def wait_a(c):
        slots = a_in.at[pl.ds(pl.multiple_of(c * 512, 512), 512)]
        pltpu.make_async_copy(slots, slots, a_recv.at[c]).wait()

    @scoped
    def transform_y(c):
        bh, bl = split(a_in[pl.ds(pl.multiple_of(c * 512, 512), 512), :])
        rhs = jnp.concatenate([bh, bh, bl], axis=0)
        for ds in YPARTS:
            blocks = [(zb + d) & 3 for d in ds]
            rows = [pl.ds(pl.multiple_of(b * 128, 128), 128) for b in blocks]
            high = jnp.concatenate([hh[r, :] for r in rows], axis=0)
            low = jnp.concatenate([hl[r, :] for r in rows], axis=0)
            r = dot(jnp.concatenate([high, low, high], axis=1), rhs)
            for i, (d, b) in enumerate(zip(ds, blocks)):
                target = b_out if d else b_in
                target[c * 4 + b] = r[128 * i : 128 * i + 128, :]
                if d:
                    pltpu.make_async_remote_copy(
                        src_ref=b_out.at[c * 4 + b],
                        dst_ref=b_in.at[c * 4 + zb],
                        send_sem=b_send,
                        recv_sem=b_recv.at[c],
                        device_id=(ya, b),
                        device_id_type=MESH,
                    ).start()

    @scoped
    def wait_b(c):
        slots = b_in.at[pl.ds(c * 4, 3)]
        pltpu.make_async_copy(slots, slots, b_recv.at[c]).wait()

    @scoped
    def transform_z(c):
        ah, al = split(jnp.concatenate([b_in[c * 4 + b] for b in range(4)], axis=1))
        lhs = jnp.concatenate([ah, ah, al], axis=1)
        column = ycol[...] + sx[ya * 16 + c]
        for k in range(2):
            cols = slice(256 * k, 256 * k + 256)
            rhs = jnp.concatenate([hh[:, cols], hl[:, cols], hh[:, cols]], axis=0)
            r = dot(lhs, rhs)
            for j in range(2):
                n = 2 * k + j
                scale = lax.rsqrt(column + sz[pl.ds(n, 1), :])
                out[c, :, 128 * n : 128 * n + 128] = r[:, 128 * j : 128 * j + 128] * scale

    rows = 32 * EARLY
    with jax.named_scope("early"):
        for g in range(4):
            bhs, bls = [], []
            landed = xin.at[pl.ds(4 * g, 4)]
            with jax.named_scope(f'ld{g}'):
                pltpu.make_async_copy(landed, landed, load_sem.at[g]).wait()
            for y in range(4 * g, 4 * g + 4):
                high, low = split(xin[y])
                xh[y] = high
                xl[y] = low
                bhs.append(high)
                bls.append(low)
            if g == 0:
                with jax.named_scope('tab'):
                    tables[0].wait()
            bh, bl = jnp.concatenate(bhs, axis=1), jnp.concatenate(bls, axis=1)
            both = dot(h1[...], bh)
            r = both[:rows] + (both[rows:] + dot(h1[pl.ds(0, rows), :], bl))
            for k in range(4):
                a_early[pl.ds(4 * g + k, rows, stride=16), :] = r[:, 128 * k : 128 * k + 128]
    with jax.named_scope("barrier_wait"):
        pl.semaphore_wait(barrier, 34)
    for c in range(EARLY):
        send_a(c)
    for t in tables[1:]:
        t.wait()
    with jax.named_scope("rest"):

        @pl.loop(0, 8, unroll=4)
        def _(g):
            bh = jnp.concatenate([xh[2 * g + k] for k in range(2)], axis=1)
            bl = jnp.concatenate([xl[2 * g + k] for k in range(2)], axis=1)
            rhs = jnp.concatenate([bh, bh, bl], axis=0)
            for p in range(1):
                rows = slice(512 * p, 512 * p + 512)
                r = dot(jnp.concatenate([hh[rows, :], hl[rows, :], hh[rows, :]], axis=1), rhs)
                for k in range(2):
                    a_out[pl.ds(512 * 16 * p + 2 * g + k, 512, stride=16), :] = r[:, 128 * k : 128 * k + 128]

    @pl.loop(EARLY, AHEAD)
    def _(c):
        send_a(c)

    ycol[...] = jnp.transpose(jnp.broadcast_to(sy[pl.ds(zb, 1), :], (128, 128)))

    @pl.loop(0, 16)
    def _(c):
        wait_a(c)
        transform_y(c)

        @pl.when(c + AHEAD < 16)
        def _():
            send_a(c + AHEAD)

        @pl.when(c >= LAG)
        def _():
            wait_b(c - LAG)
            transform_z(c - LAG)

    @pl.loop(16 - LAG, 16)
    def _(c):
        wait_b(c)
        transform_z(c)

    with jax.named_scope("drain"):

        sent = a_in.at[pl.ds(0, 16 * 31 * 16)]
        pltpu.make_async_copy(sent, sent, a_send).wait()
        sent = b_out.at[pl.ds(0, 16 * 3)]
        pltpu.make_async_copy(sent, sent, b_send).wait()


def body(source, symbol_x, symbol_y, symbol_z):
    high, low = halves(table())
    order = np.array([a * 16 + c for c in range(EARLY) for a in range(32)])
    stacked = np.concatenate([high[order], low[order]])
    any_space = pl.BlockSpec(memory_space=pl.ANY)
    f32, bf16 = jnp.float32, jnp.bfloat16
    return pl.pallas_call(
        kernel,
        out_shape=pltpu.VMEM((16, 128, 512), f32),
        in_specs=[any_space] * 7,
        out_specs=pl.BlockSpec(memory_space=pltpu.VMEM),
        scratch_shapes=[
            pltpu.VMEM((16, 512, 128), f32),
            pltpu.VMEM((16, 512, 128), bf16),
            pltpu.VMEM((16, 512, 128), bf16),
            pltpu.VMEM(stacked.shape, bf16),
            pltpu.VMEM((512, 512), bf16),
            pltpu.VMEM((512, 512), bf16),
            pltpu.VMEM((len(order) * 16, 128), f32),
            pltpu.VMEM((8192, 128), f32),
            pltpu.VMEM((8192, 128), f32),
            pltpu.VMEM((64, 128, 128), f32),
            pltpu.VMEM((64, 128, 128), f32),
            pltpu.VMEM((128, 128), f32),
            pltpu.SMEM((512,), f32),
            pltpu.VMEM((4, 128), f32),
            pltpu.VMEM((4, 128), f32),
            pltpu.SemaphoreType.DMA((4,)),
            pltpu.SemaphoreType.DMA((6,)),
            pltpu.SemaphoreType.DMA,
            pltpu.SemaphoreType.DMA((16,)),
            pltpu.SemaphoreType.DMA,
            pltpu.SemaphoreType.DMA((16,)),
        ],
        compiler_params=pltpu.CompilerParams(
            collective_id=0, has_side_effects=True, vmem_limit_bytes=67043328 - 4 * 1024 * 1024 - 65536
        ),
    )(
        source.reshape(512, 16, 1, 128),
        jnp.asarray(stacked),
        jnp.asarray(high),
        jnp.asarray(low),
        symbol_x,
        symbol_y.reshape(4, 128),
        symbol_z.reshape(4, 128),
    )


def solution(mesh):
    placed = (P(None, "ya", "zb"), P(), P(), P())
    return jax.shard_map(
        body, mesh=mesh, in_specs=placed, out_specs=P("ya", "zb", None), check_vma=False
    )
```

```python
import functools

import jax
import jax.numpy as jnp
import ml_dtypes
import numpy as np
from jax import lax
from jax.experimental import pallas as pl
from jax.experimental.pallas import tpu as pltpu
from jax.sharding import PartitionSpec as P

MESH = pl.DeviceIdType.MESH


def scoped(f):
    def g(*args):
        with jax.named_scope(f.__name__):
            return f(*args)

    return g

N = 512
FAR = (10, 11, 14, 9, 6, 5, 7, 13, 15, 8, 2, 1, 4, 3, 12)
EARLY = 2
YPARTS = ((1, 3), (2, 0))
AHEAD = 3
LAG = 2
GROUPS = ((0, 4), (4, 4), (8, 4), (12, 4))


def table():
    rank = np.arange(1, N + 1)
    angle = np.pi * (rank[:, None] * rank[None, :] % (2 * N + 2)) / (N + 1)
    return np.sqrt(2.0 / (N + 1)) * np.sin(angle)


def halves(h):
    high = h.astype(ml_dtypes.bfloat16)
    return high, (h - high.astype(np.float64)).astype(ml_dtypes.bfloat16)


def split(v):
    high = v.astype(jnp.bfloat16)
    return high, (v - high.astype(jnp.float32)).astype(jnp.bfloat16)


def dot(a, b):
    return jnp.dot(a, b, preferred_element_type=jnp.float32)


def kernel(
    src, h1_hbm, hh_hbm, hl_hbm, sx_hbm, sy_hbm, sz_hbm, out,
    xin, xh, xl, h1, hh, hl, a_early, a_out, a_in, b_out, b_in, ycol, sx, sy, sz,
    load_sem, table_sem, a_send, a_recv, b_send, b_recv,
):
    ya, zb = lax.axis_index("ya"), lax.axis_index("zb")

    def load(y):
        group = max(g for g in range(len(GROUPS)) if GROUPS[g][0] <= y)
        return pltpu.make_async_copy(src.at[:, y, 0, :], xin.at[y], load_sem.at[group])

    tables = [
        pltpu.make_async_copy(s, d, table_sem.at[k])
        for k, (s, d) in enumerate(
            ((h1_hbm, h1), (hh_hbm, hh), (hl_hbm, hl), (sx_hbm, sx), (sy_hbm, sy), (sz_hbm, sz))
        )
    ]
    tables[0].start()
    for y in range(4):
        load(y).start()

    z0, y0 = ya >> 3, (ya >> 1) & 3
    peers = [z * 8 + y * 2 + k for k in (1, 0) for z in (0, 1, 3, 2) for y in (0, 1, 3, 2)]

    barrier = pltpu.get_barrier_semaphore()
    for peer in peers:

        @pl.when(peer != ya)
        def _():
            pl.semaphore_signal(barrier, inc=1, device_id=(peer, zb), device_id_type=MESH)

    for d in (1, 3, 2):
        pl.semaphore_signal(barrier, inc=1, device_id=(ya, (zb + d) & 3), device_id_type=MESH)
    for y in range(4, 16):
        load(y).start()

    def a_slot(c, who):
        return a_in.at[pl.ds(pl.multiple_of(c * 512 + who * 16, 16), 16)]

    def a_source(c, who):
        if isinstance(c, int) and c < EARLY:
            return a_early.at[pl.ds(pl.multiple_of(c * 512 + who * 16, 16), 16)]
        return a_out.at[pl.ds(pl.multiple_of(who * 256 + c * 16, 16), 16)]

    @scoped
    def send_a(c):
        pltpu.make_async_copy(a_source(c, ya), a_slot(c, ya), a_recv.at[c]).start()
        for peer in peers:

            @pl.when(peer != ya)
            def _():
                pltpu.make_async_remote_copy(
                    src_ref=a_source(c, peer),
                    dst_ref=a_slot(c, ya),
                    send_sem=a_send,
                    recv_sem=a_recv.at[c],
                    device_id=(peer, zb),
                    device_id_type=MESH,
                ).start()

    @scoped
    def wait_a(c):
        slots = a_in.at[pl.ds(pl.multiple_of(c * 512, 512), 512)]
        pltpu.make_async_copy(slots, slots, a_recv.at[c]).wait()

    @scoped
    def transform_y(c):
        bh, bl = split(a_in[pl.ds(pl.multiple_of(c * 512, 512), 512), :])
        rhs = jnp.concatenate([bh, bh, bl], axis=0)
        for ds in YPARTS:
            blocks = [(zb + d) & 3 for d in ds]
            rows = [pl.ds(pl.multiple_of(b * 128, 128), 128) for b in blocks]
            high = jnp.concatenate([hh[r, :] for r in rows], axis=0)
            low = jnp.concatenate([hl[r, :] for r in rows], axis=0)
            r = dot(jnp.concatenate([high, low, high], axis=1), rhs)
            for i, (d, b) in enumerate(zip(ds, blocks)):
                target = b_out if d else b_in
                target[c * 4 + b] = r[128 * i : 128 * i + 128, :]
                if d:
                    pltpu.make_async_remote_copy(
                        src_ref=b_out.at[c * 4 + b],
                        dst_ref=b_in.at[c * 4 + zb],
                        send_sem=b_send,
                        recv_sem=b_recv.at[c],
                        device_id=(ya, b),
                        device_id_type=MESH,
                    ).start()

    @scoped
    def wait_b(c):
        slots = b_in.at[pl.ds(c * 4, 3)]
        pltpu.make_async_copy(slots, slots, b_recv.at[c]).wait()

    @scoped
    def transform_z(c):
        ah, al = split(jnp.concatenate([b_in[c * 4 + b] for b in range(4)], axis=1))
        lhs = jnp.concatenate([ah, ah, al], axis=1)
        column = ycol[...] + sx[ya * 16 + c]
        for k in range(2):
            cols = slice(256 * k, 256 * k + 256)
            rhs = jnp.concatenate([hh[:, cols], hl[:, cols], hh[:, cols]], axis=0)
            r = dot(lhs, rhs)
            for j in range(2):
                n = 2 * k + j
                scale = lax.rsqrt(column + sz[pl.ds(n, 1), :])
                out[c, :, 128 * n : 128 * n + 128] = r[:, 128 * j : 128 * j + 128] * scale

    rows = 32 * EARLY
    with jax.named_scope("early"):
        for g, (y0, ny) in enumerate(GROUPS):
            bhs, bls = [], []
            landed = xin.at[pl.ds(y0, ny)]
            with jax.named_scope(f"ld{g}"):
                pltpu.make_async_copy(landed, landed, load_sem.at[g]).wait()
            for y in range(y0, y0 + ny):
                high, low = split(xin[y])
                xh[y] = high
                xl[y] = low
                bhs.append(high)
                bls.append(low)
            if g == 2:
                for t in tables[1:]:
                    t.start()
            if g == 0:
                with jax.named_scope("tab"):
                    tables[0].wait()
            bh, bl = jnp.concatenate(bhs, axis=1), jnp.concatenate(bls, axis=1)
            both = dot(h1[...], bh)
            r = both[:rows] + (both[rows:] + dot(h1[pl.ds(0, rows), :], bl))
            for k in range(ny):
                a_early[pl.ds(y0 + k, rows, stride=16), :] = r[:, 128 * k : 128 * k + 128]
    with jax.named_scope("barrier_wait"):
        pl.semaphore_wait(barrier, 34)
    for c in range(EARLY):
        send_a(c)
    for t in tables[1:]:
        t.wait()
    with jax.named_scope("rest"):

        @pl.loop(0, 8, unroll=4)
        def _(g):
            bh = jnp.concatenate([xh[2 * g + k] for k in range(2)], axis=1)
            bl = jnp.concatenate([xl[2 * g + k] for k in range(2)], axis=1)
            rhs = jnp.concatenate([bh, bh, bl], axis=0)
            for p in range(1):
                rows = slice(512 * p, 512 * p + 512)
                r = dot(jnp.concatenate([hh[rows, :], hl[rows, :], hh[rows, :]], axis=1), rhs)
                for k in range(2):
                    a_out[pl.ds(512 * 16 * p + 2 * g + k, 512, stride=16), :] = r[:, 128 * k : 128 * k + 128]

    @pl.loop(EARLY, AHEAD)
    def _(c):
        send_a(c)

    ycol[...] = jnp.transpose(jnp.broadcast_to(sy[pl.ds(zb, 1), :], (128, 128)))

    @pl.loop(0, 16)
    def _(c):
        wait_a(c)
        transform_y(c)

        @pl.when(c + AHEAD < 16)
        def _():
            send_a(c + AHEAD)

        @pl.when(c >= LAG)
        def _():
            wait_b(c - LAG)
            transform_z(c - LAG)

    @pl.loop(16 - LAG, 16)
    def _(c):
        wait_b(c)
        transform_z(c)

    with jax.named_scope("drain"):

        sent = a_in.at[pl.ds(0, 16 * 31 * 16)]
        pltpu.make_async_copy(sent, sent, a_send).wait()
        sent = b_out.at[pl.ds(0, 16 * 3)]
        pltpu.make_async_copy(sent, sent, b_send).wait()


def body(source, symbol_x, symbol_y, symbol_z):
    high, low = halves(table())
    order = np.array([a * 16 + c for c in range(EARLY) for a in range(32)])
    stacked = np.concatenate([high[order], low[order]])
    any_space = pl.BlockSpec(memory_space=pl.ANY)
    f32, bf16 = jnp.float32, jnp.bfloat16
    return pl.pallas_call(
        kernel,
        out_shape=pltpu.VMEM((16, 128, 512), f32),
        in_specs=[any_space] * 7,
        out_specs=pl.BlockSpec(memory_space=pltpu.VMEM),
        scratch_shapes=[
            pltpu.VMEM((16, 512, 128), f32),
            pltpu.VMEM((16, 512, 128), bf16),
            pltpu.VMEM((16, 512, 128), bf16),
            pltpu.VMEM(stacked.shape, bf16),
            pltpu.VMEM((512, 512), bf16),
            pltpu.VMEM((512, 512), bf16),
            pltpu.VMEM((len(order) * 16, 128), f32),
            pltpu.VMEM((8192, 128), f32),
            pltpu.VMEM((8192, 128), f32),
            pltpu.VMEM((64, 128, 128), f32),
            pltpu.VMEM((64, 128, 128), f32),
            pltpu.VMEM((128, 128), f32),
            pltpu.SMEM((512,), f32),
            pltpu.VMEM((4, 128), f32),
            pltpu.VMEM((4, 128), f32),
            pltpu.SemaphoreType.DMA((len(GROUPS),)),
            pltpu.SemaphoreType.DMA((6,)),
            pltpu.SemaphoreType.DMA,
            pltpu.SemaphoreType.DMA((16,)),
            pltpu.SemaphoreType.DMA,
            pltpu.SemaphoreType.DMA((16,)),
        ],
        compiler_params=pltpu.CompilerParams(
            collective_id=0, has_side_effects=True, vmem_limit_bytes=67043328 - 4 * 1024 * 1024 - 65536
        ),
    )(
        source.reshape(512, 16, 1, 128),
        jnp.asarray(stacked),
        jnp.asarray(high),
        jnp.asarray(low),
        symbol_x,
        symbol_y.reshape(4, 128),
        symbol_z.reshape(4, 128),
    )


def solution(mesh):
    placed = (P(None, "ya", "zb"), P(), P(), P())
    return jax.shard_map(
        body, mesh=mesh, in_specs=placed, out_specs=P("ya", "zb", None), check_vma=False
    )
```

```python
import functools

import jax
import jax.numpy as jnp
import ml_dtypes
import numpy as np
from jax import lax
from jax.experimental import pallas as pl
from jax.experimental.pallas import tpu as pltpu
from jax.sharding import PartitionSpec as P

MESH = pl.DeviceIdType.MESH


def scoped(f):
    def g(*args):
        with jax.named_scope(f.__name__):
            return f(*args)

    return g

N = 512
FAR = (10, 11, 14, 9, 6, 5, 7, 13, 15, 8, 2, 1, 4, 3, 12)
EARLY = 2
YPARTS = ((1, 3), (2, 0))
AHEAD = 3
LAG = 2
FINAL = 1
GROUPS = ((0, 4), (4, 4), (8, 4), (12, 4))


def table():
    rank = np.arange(1, N + 1)
    angle = np.pi * (rank[:, None] * rank[None, :] % (2 * N + 2)) / (N + 1)
    return np.sqrt(2.0 / (N + 1)) * np.sin(angle)


def halves(h):
    high = h.astype(ml_dtypes.bfloat16)
    return high, (h - high.astype(np.float64)).astype(ml_dtypes.bfloat16)


def split(v):
    high = v.astype(jnp.bfloat16)
    return high, (v - high.astype(jnp.float32)).astype(jnp.bfloat16)


def dot(a, b):
    return jnp.dot(a, b, preferred_element_type=jnp.float32)


def kernel(
    src, h1_hbm, hh_hbm, hl_hbm, sx_hbm, sy_hbm, sz_hbm, out, b_in, hh, hl,
    xin, xh, xl, h1, a_early, a_out, a_in, b_out, ycol, sx, sy, sz,
    load_sem, table_sem, a_send, a_recv, b_send, b_recv,
):
    ya, zb = lax.axis_index("ya"), lax.axis_index("zb")

    def load(y):
        group = max(g for g in range(len(GROUPS)) if GROUPS[g][0] <= y)
        return pltpu.make_async_copy(src.at[:, y, 0, :], xin.at[y], load_sem.at[group])

    tables = [
        pltpu.make_async_copy(s, d, table_sem.at[k])
        for k, (s, d) in enumerate(
            ((h1_hbm, h1), (hh_hbm, hh), (hl_hbm, hl), (sx_hbm, sx), (sy_hbm, sy), (sz_hbm, sz))
        )
    ]
    tables[0].start()
    for y in range(4):
        load(y).start()

    z0, y0 = ya >> 3, (ya >> 1) & 3
    peers = [z * 8 + y * 2 + k for k in (1, 0) for z in (0, 1, 3, 2) for y in (0, 1, 3, 2)]

    barrier = pltpu.get_barrier_semaphore()
    for peer in peers:

        @pl.when(peer != ya)
        def _():
            pl.semaphore_signal(barrier, inc=1, device_id=(peer, zb), device_id_type=MESH)

    for d in (1, 3, 2):
        pl.semaphore_signal(barrier, inc=1, device_id=(ya, (zb + d) & 3), device_id_type=MESH)
    for y in range(4, 16):
        load(y).start()

    def a_slot(c, who):
        return a_in.at[pl.ds(pl.multiple_of(c * 512 + who * 16, 16), 16)]

    def a_source(c, who):
        if isinstance(c, int) and c < EARLY:
            return a_early.at[pl.ds(pl.multiple_of(c * 512 + who * 16, 16), 16)]
        return a_out.at[pl.ds(pl.multiple_of(who * 256 + c * 16, 16), 16)]

    @scoped
    def send_a(c):
        pltpu.make_async_copy(a_source(c, ya), a_slot(c, ya), a_recv.at[c]).start()
        for peer in peers:

            @pl.when(peer != ya)
            def _():
                pltpu.make_async_remote_copy(
                    src_ref=a_source(c, peer),
                    dst_ref=a_slot(c, ya),
                    send_sem=a_send,
                    recv_sem=a_recv.at[c],
                    device_id=(peer, zb),
                    device_id_type=MESH,
                ).start()

    @scoped
    def wait_a(c):
        slots = a_in.at[pl.ds(pl.multiple_of(c * 512, 512), 512)]
        pltpu.make_async_copy(slots, slots, a_recv.at[c]).wait()

    @scoped
    def transform_y(c):
        bh, bl = split(a_in[pl.ds(pl.multiple_of(c * 512, 512), 512), :])
        rhs = jnp.concatenate([bh, bh, bl], axis=0)
        for blocks in ((0, 1), (3, 2)):
            rows = [slice(128 * b, 128 * b + 128) for b in blocks]
            high = jnp.concatenate([hh[r, :] for r in rows], axis=0)
            low = jnp.concatenate([hl[r, :] for r in rows], axis=0)
            r = dot(jnp.concatenate([high, low, high], axis=1), rhs)
            for i, b in enumerate(blocks):
                b_out[c * 4 + b] = r[128 * i : 128 * i + 128, :]

                @pl.when(zb != b)
                def _():
                    pltpu.make_async_remote_copy(
                        src_ref=b_out.at[c * 4 + b],
                        dst_ref=b_in.at[c * 4 + zb],
                        send_sem=b_send,
                        recv_sem=b_recv.at[c],
                        device_id=(ya, b),
                        device_id_type=MESH,
                    ).start()

                @pl.when(zb == b)
                def _():
                    pltpu.make_async_copy(b_out.at[c * 4 + b], b_in.at[c * 4 + b], b_recv.at[c]).start()

    @scoped
    def wait_b(c):
        slots = b_in.at[pl.ds(c * 4, 4)]
        pltpu.make_async_copy(slots, slots, b_recv.at[c]).wait()

    @scoped
    def transform_z(c):
        ah, al = split(jnp.concatenate([b_in[c * 4 + b] for b in range(4)], axis=1))
        lhs = jnp.concatenate([ah, ah, al], axis=1)
        column = ycol[...] + sx[ya * 16 + c]
        for k in range(2):
            cols = slice(256 * k, 256 * k + 256)
            rhs = jnp.concatenate([hh[:, cols], hl[:, cols], hh[:, cols]], axis=0)
            r = dot(lhs, rhs)
            for j in range(2):
                n = 2 * k + j
                scale = lax.rsqrt(column + sz[pl.ds(n, 1), :])
                out[c, :, 128 * n : 128 * n + 128] = r[:, 128 * j : 128 * j + 128] * scale

    rows = 32 * EARLY
    with jax.named_scope("early"):
        for g, (y0, ny) in enumerate(GROUPS):
            bhs, bls = [], []
            landed = xin.at[pl.ds(y0, ny)]
            with jax.named_scope(f"ld{g}"):
                pltpu.make_async_copy(landed, landed, load_sem.at[g]).wait()
            for y in range(y0, y0 + ny):
                high, low = split(xin[y])
                xh[y] = high
                xl[y] = low
                bhs.append(high)
                bls.append(low)
            if g == 2:
                for t in tables[1:]:
                    t.start()
            if g == 0:
                with jax.named_scope("tab"):
                    tables[0].wait()
            bh, bl = jnp.concatenate(bhs, axis=1), jnp.concatenate(bls, axis=1)
            both = dot(h1[...], bh)
            r = both[:rows] + (both[rows:] + dot(h1[pl.ds(0, rows), :], bl))
            for k in range(ny):
                a_early[pl.ds(y0 + k, rows, stride=16), :] = r[:, 128 * k : 128 * k + 128]
    with jax.named_scope("barrier_wait"):
        pl.semaphore_wait(barrier, 34)
    for c in range(EARLY):
        send_a(c)
    for t in tables[1:]:
        t.wait()
    with jax.named_scope("rest"):

        @pl.loop(0, 8, unroll=4)
        def _(g):
            bh = jnp.concatenate([xh[2 * g + k] for k in range(2)], axis=1)
            bl = jnp.concatenate([xl[2 * g + k] for k in range(2)], axis=1)
            rhs = jnp.concatenate([bh, bh, bl], axis=0)
            for p in range(1):
                rows = slice(512 * p, 512 * p + 512)
                r = dot(jnp.concatenate([hh[rows, :], hl[rows, :], hh[rows, :]], axis=1), rhs)
                for k in range(2):
                    a_out[pl.ds(512 * 16 * p + 2 * g + k, 512, stride=16), :] = r[:, 128 * k : 128 * k + 128]

    @pl.loop(EARLY, AHEAD)
    def _(c):
        send_a(c)

    ycol[...] = jnp.transpose(jnp.broadcast_to(sy[pl.ds(zb, 1), :], (128, 128)))

    @pl.loop(0, 16)
    def _(c):
        wait_a(c)
        transform_y(c)

        @pl.when(c + AHEAD < 16)
        def _():
            send_a(c + AHEAD)

        @pl.when(c >= LAG)
        def _():
            wait_b(c - LAG)
            transform_z(c - LAG)

    @pl.loop(16 - LAG, 16)
    def _(c):
        wait_b(c)

        @pl.when(c < 15)
        def _():
            transform_z(c)

    with jax.named_scope("drain"):

        sent = a_in.at[pl.ds(0, 16 * 31 * 16)]
        pltpu.make_async_copy(sent, sent, a_send).wait()
        sent = b_out.at[pl.ds(0, 16 * 3)]
        pltpu.make_async_copy(sent, sent, b_send).wait()


def finish(done, b_in, hh, hl, sx_hbm, sy_hbm, sz_hbm, out, last, sx, sy, sz, out_sem, sem):
    ya, zb = lax.axis_index("ya"), lax.axis_index("zb")
    loads = [pltpu.make_async_copy(s, d, sem.at[k]) for k, (s, d) in enumerate(((sx_hbm, sx), (sy_hbm, sy), (sz_hbm, sz)))]
    for t in loads:
        t.start()
    first = 16 - FINAL
    pltpu.make_async_copy(done.at[pl.ds(0, first)], out.at[pl.ds(0, first)], out_sem).start()
    for t in loads:
        t.wait()
    ycol = jnp.transpose(jnp.broadcast_to(sy[pl.ds(zb, 1), :], (128, 128)))
    for i in range(FINAL):
        c = first + i
        ah, al = split(jnp.concatenate([b_in[c * 4 + b] for b in range(4)], axis=1))
        lhs = jnp.concatenate([ah, ah, al], axis=1)
        column = ycol + sx[ya * 16 + c]
        for k in range(2):
            cols = slice(256 * k, 256 * k + 256)
            rhs = jnp.concatenate([hh[:, cols], hl[:, cols], hh[:, cols]], axis=0)
            r = dot(lhs, rhs)
            for j in range(2):
                n = 2 * k + j
                scale = lax.rsqrt(column + sz[pl.ds(n, 1), :])
                last[i, :, 128 * n : 128 * n + 128] = r[:, 128 * j : 128 * j + 128] * scale
        pltpu.make_async_copy(last.at[i], out.at[c], out_sem).start()
    pltpu.make_async_copy(out, out, out_sem).wait()


def body(source, symbol_x, symbol_y, symbol_z):
    high, low = halves(table())
    order = np.array([a * 16 + c for c in range(EARLY) for a in range(32)])
    stacked = np.concatenate([high[order], low[order]])
    any_space = pl.BlockSpec(memory_space=pl.ANY)
    f32, bf16 = jnp.float32, jnp.bfloat16
    done, b_in, hh, hl = pl.pallas_call(
        kernel,
        out_shape=(
            pltpu.VMEM((16, 128, 512), f32),
            pltpu.VMEM((64, 128, 128), f32),
            pltpu.VMEM((512, 512), bf16),
            pltpu.VMEM((512, 512), bf16),
        ),
        in_specs=[any_space] * 7,
        out_specs=(pl.BlockSpec(memory_space=pltpu.VMEM),) * 4,
        scratch_shapes=[
            pltpu.VMEM((16, 512, 128), f32),
            pltpu.VMEM((16, 512, 128), bf16),
            pltpu.VMEM((16, 512, 128), bf16),
            pltpu.VMEM(stacked.shape, bf16),
            pltpu.VMEM((len(order) * 16, 128), f32),
            pltpu.VMEM((8192, 128), f32),
            pltpu.VMEM((8192, 128), f32),
            pltpu.VMEM((64, 128, 128), f32),
            pltpu.VMEM((128, 128), f32),
            pltpu.SMEM((512,), f32),
            pltpu.VMEM((4, 128), f32),
            pltpu.VMEM((4, 128), f32),
            pltpu.SemaphoreType.DMA((len(GROUPS),)),
            pltpu.SemaphoreType.DMA((6,)),
            pltpu.SemaphoreType.DMA,
            pltpu.SemaphoreType.DMA((16,)),
            pltpu.SemaphoreType.DMA,
            pltpu.SemaphoreType.DMA((16,)),
        ],
        compiler_params=pltpu.CompilerParams(
            collective_id=0, has_side_effects=True, vmem_limit_bytes=67043328 - 9 * 1024 * 1024 - 65536
        ),
    )(
        source.reshape(512, 16, 1, 128),
        jnp.asarray(stacked),
        jnp.asarray(high),
        jnp.asarray(low),
        symbol_x,
        symbol_y.reshape(4, 128),
        symbol_z.reshape(4, 128),
    )
    return pl.pallas_call(
        finish,
        out_shape=jax.ShapeDtypeStruct((16, 128, 512), f32),
        in_specs=[pl.BlockSpec(memory_space=pltpu.VMEM)] * 4 + [any_space] * 3,
        out_specs=any_space,
        scratch_shapes=[
            pltpu.VMEM((FINAL, 128, 512), f32),
            pltpu.SMEM((512,), f32),
            pltpu.VMEM((4, 128), f32),
            pltpu.VMEM((4, 128), f32),
            pltpu.SemaphoreType.DMA,
            pltpu.SemaphoreType.DMA((3,)),
        ],
        compiler_params=pltpu.CompilerParams(vmem_limit_bytes=32 * 1024 * 1024),
    )(done, b_in, hh, hl, symbol_x, symbol_y.reshape(4, 128), symbol_z.reshape(4, 128))


def solution(mesh):
    placed = (P(None, "ya", "zb"), P(), P(), P())
    return jax.shard_map(
        body, mesh=mesh, in_specs=placed, out_specs=P("ya", "zb", None), check_vma=False
    )
```

```python
import functools

import jax
import jax.numpy as jnp
import ml_dtypes
import numpy as np
from jax import lax
from jax.experimental import pallas as pl
from jax.experimental.pallas import tpu as pltpu
from jax.sharding import PartitionSpec as P

MESH = pl.DeviceIdType.MESH


def scoped(f):
    def g(*args):
        with jax.named_scope(f.__name__):
            return f(*args)

    return g

N = 512
FAR = (10, 11, 14, 9, 6, 5, 7, 13, 15, 8, 2, 1, 4, 3, 12)
EARLY = 2
YPARTS = ((1, 3), (2, 0))
AHEAD = 3
LAG = 2
FINAL = 1
GROUPS = ((0, 4), (4, 4), (8, 4), (12, 4))


def table():
    rank = np.arange(1, N + 1)
    angle = np.pi * (rank[:, None] * rank[None, :] % (2 * N + 2)) / (N + 1)
    return np.sqrt(2.0 / (N + 1)) * np.sin(angle)


def halves(h):
    high = h.astype(ml_dtypes.bfloat16)
    return high, (h - high.astype(np.float64)).astype(ml_dtypes.bfloat16)


def split(v):
    high = v.astype(jnp.bfloat16)
    return high, (v - high.astype(jnp.float32)).astype(jnp.bfloat16)


def dot(a, b):
    return jnp.dot(a, b, preferred_element_type=jnp.float32)


def kernel(
    src, h1_hbm, hh_hbm, hl_hbm, sx_hbm, sy_hbm, sz_hbm, out, b_in, hh, hl,
    xin, xh, xl, h1, a_early, a_out, a_in, b_out, ycol, sx, sy, sz,
    load_sem, table_sem, a_send, a_recv, b_send, b_recv,
):
    ya, zb = lax.axis_index("ya"), lax.axis_index("zb")

    def load(y):
        group = max(g for g in range(len(GROUPS)) if GROUPS[g][0] <= y)
        return pltpu.make_async_copy(src.at[:, y, 0, :], xin.at[y], load_sem.at[group])

    tables = [
        pltpu.make_async_copy(s, d, table_sem.at[k])
        for k, (s, d) in enumerate(
            ((h1_hbm, h1), (hh_hbm, hh), (hl_hbm, hl), (sx_hbm, sx), (sy_hbm, sy), (sz_hbm, sz))
        )
    ]
    tables[0].start()
    for y in range(4):
        load(y).start()

    z0, y0 = ya >> 3, (ya >> 1) & 3
    peers = [z * 8 + y * 2 + k for k in (1, 0) for z in (0, 1, 3, 2) for y in (0, 1, 3, 2)]

    barrier = pltpu.get_barrier_semaphore()
    for peer in peers:

        @pl.when(peer != ya)
        def _():
            pl.semaphore_signal(barrier, inc=1, device_id=(peer, zb), device_id_type=MESH)

    for d in (1, 3, 2):
        pl.semaphore_signal(barrier, inc=1, device_id=(ya, (zb + d) & 3), device_id_type=MESH)
    for y in range(4, 16):
        load(y).start()

    def a_slot(c, who):
        return a_in.at[pl.ds(pl.multiple_of(c * 512 + who * 16, 16), 16)]

    def a_source(c, who):
        if isinstance(c, int) and c < EARLY:
            return a_early.at[pl.ds(pl.multiple_of(c * 512 + who * 16, 16), 16)]
        return a_out.at[pl.ds(pl.multiple_of(who * 256 + c * 16, 16), 16)]

    @scoped
    def send_a(c):
        pltpu.make_async_copy(a_source(c, ya), a_slot(c, ya), a_recv.at[c]).start()
        for peer in peers:

            @pl.when(peer != ya)
            def _():
                pltpu.make_async_remote_copy(
                    src_ref=a_source(c, peer),
                    dst_ref=a_slot(c, ya),
                    send_sem=a_send,
                    recv_sem=a_recv.at[c],
                    device_id=(peer, zb),
                    device_id_type=MESH,
                ).start()

    @scoped
    def wait_a(c):
        slots = a_in.at[pl.ds(pl.multiple_of(c * 512, 512), 512)]
        pltpu.make_async_copy(slots, slots, a_recv.at[c]).wait()

    @scoped
    def transform_y(c):
        bh, bl = split(a_in[pl.ds(pl.multiple_of(c * 512, 512), 512), :])
        rhs = jnp.concatenate([bh, bh, bl], axis=0)
        for blocks in ((0, 1), (3, 2)):
            rows = [slice(128 * b, 128 * b + 128) for b in blocks]
            high = jnp.concatenate([hh[r, :] for r in rows], axis=0)
            low = jnp.concatenate([hl[r, :] for r in rows], axis=0)
            r = dot(jnp.concatenate([high, low, high], axis=1), rhs)
            for i, b in enumerate(blocks):
                b_out[c * 4 + b] = r[128 * i : 128 * i + 128, :]

                @pl.when(zb != b)
                def _():
                    pltpu.make_async_remote_copy(
                        src_ref=b_out.at[c * 4 + b],
                        dst_ref=b_in.at[c * 4 + zb],
                        send_sem=b_send,
                        recv_sem=b_recv.at[c],
                        device_id=(ya, b),
                        device_id_type=MESH,
                    ).start()

                @pl.when(zb == b)
                def _():
                    pltpu.make_async_copy(b_out.at[c * 4 + b], b_in.at[c * 4 + b], b_recv.at[c]).start()

    @scoped
    def wait_b(c):
        slots = b_in.at[pl.ds(c * 4, 4)]
        pltpu.make_async_copy(slots, slots, b_recv.at[c]).wait()

    @scoped
    def transform_z(c):
        ah, al = split(jnp.concatenate([b_in[c * 4 + b] for b in range(4)], axis=1))
        lhs = jnp.concatenate([ah, ah, al], axis=1)
        column = ycol[...] + sx[ya * 16 + c]
        for k in range(2):
            cols = slice(256 * k, 256 * k + 256)
            rhs = jnp.concatenate([hh[:, cols], hl[:, cols], hh[:, cols]], axis=0)
            r = dot(lhs, rhs)
            for j in range(2):
                n = 2 * k + j
                scale = lax.rsqrt(column + sz[pl.ds(n, 1), :])
                out[c, :, 128 * n : 128 * n + 128] = r[:, 128 * j : 128 * j + 128] * scale

    rows = 32 * EARLY
    with jax.named_scope("early"):
        for g, (y0, ny) in enumerate(GROUPS):
            bhs, bls = [], []
            landed = xin.at[pl.ds(y0, ny)]
            with jax.named_scope(f"ld{g}"):
                pltpu.make_async_copy(landed, landed, load_sem.at[g]).wait()
            for y in range(y0, y0 + ny):
                high, low = split(xin[y])
                xh[y] = high
                xl[y] = low
                bhs.append(high)
                bls.append(low)
            if g == 2:
                for t in tables[1:]:
                    t.start()
            if g == 0:
                with jax.named_scope("tab"):
                    tables[0].wait()
            bh, bl = jnp.concatenate(bhs, axis=1), jnp.concatenate(bls, axis=1)
            both = dot(h1[...], bh)
            r = both[:rows] + (both[rows:] + dot(h1[pl.ds(0, rows), :], bl))
            for k in range(ny):
                a_early[pl.ds(y0 + k, rows, stride=16), :] = r[:, 128 * k : 128 * k + 128]
    with jax.named_scope("barrier_wait"):
        pl.semaphore_wait(barrier, 34)
    send_a(0)
    for t in tables[1:]:
        t.wait()
    with jax.named_scope("rest"):

        @pl.loop(0, 2, unroll=2)
        def _(g):
            bh = jnp.concatenate([xh[2 * g + k] for k in range(2)], axis=1)
            bl = jnp.concatenate([xl[2 * g + k] for k in range(2)], axis=1)
            rhs = jnp.concatenate([bh, bh, bl], axis=0)
            for p in range(1):
                rows = slice(512 * p, 512 * p + 512)
                r = dot(jnp.concatenate([hh[rows, :], hl[rows, :], hh[rows, :]], axis=1), rhs)
                for k in range(2):
                    a_out[pl.ds(512 * 16 * p + 2 * g + k, 512, stride=16), :] = r[:, 128 * k : 128 * k + 128]

        send_a(1)

        @pl.loop(2, 8, unroll=3)
        def _(g):
            bh = jnp.concatenate([xh[2 * g + k] for k in range(2)], axis=1)
            bl = jnp.concatenate([xl[2 * g + k] for k in range(2)], axis=1)
            rhs = jnp.concatenate([bh, bh, bl], axis=0)
            for p in range(1):
                rows = slice(512 * p, 512 * p + 512)
                r = dot(jnp.concatenate([hh[rows, :], hl[rows, :], hh[rows, :]], axis=1), rhs)
                for k in range(2):
                    a_out[pl.ds(512 * 16 * p + 2 * g + k, 512, stride=16), :] = r[:, 128 * k : 128 * k + 128]

    @pl.loop(EARLY, AHEAD)
    def _(c):
        send_a(c)

    ycol[...] = jnp.transpose(jnp.broadcast_to(sy[pl.ds(zb, 1), :], (128, 128)))

    @pl.loop(0, 16)
    def _(c):
        wait_a(c)
        transform_y(c)

        @pl.when(c + AHEAD < 16)
        def _():
            send_a(c + AHEAD)

        @pl.when(c >= LAG)
        def _():
            wait_b(c - LAG)
            transform_z(c - LAG)

    @pl.loop(16 - LAG, 16)
    def _(c):
        wait_b(c)

        @pl.when(c < 15)
        def _():
            transform_z(c)

    with jax.named_scope("drain"):

        sent = a_in.at[pl.ds(0, 16 * 31 * 16)]
        pltpu.make_async_copy(sent, sent, a_send).wait()
        sent = b_out.at[pl.ds(0, 16 * 3)]
        pltpu.make_async_copy(sent, sent, b_send).wait()


def finish(done, b_in, hh, hl, sx_hbm, sy_hbm, sz_hbm, out, last, sx, sy, sz, out_sem, sem):
    ya, zb = lax.axis_index("ya"), lax.axis_index("zb")
    loads = [pltpu.make_async_copy(s, d, sem.at[k]) for k, (s, d) in enumerate(((sx_hbm, sx), (sy_hbm, sy), (sz_hbm, sz)))]
    for t in loads:
        t.start()
    first = 16 - FINAL
    for k in range(5):
        pltpu.make_async_copy(done.at[pl.ds(3 * k, 3)], out.at[pl.ds(3 * k, 3)], out_sem).start()
    for t in loads:
        t.wait()
    ycol = jnp.transpose(jnp.broadcast_to(sy[pl.ds(zb, 1), :], (128, 128)))
    for i in range(FINAL):
        c = first + i
        ah, al = split(jnp.concatenate([b_in[c * 4 + b] for b in range(4)], axis=1))
        lhs = jnp.concatenate([ah, ah, al], axis=1)
        column = ycol + sx[ya * 16 + c]
        for k in range(2):
            cols = slice(256 * k, 256 * k + 256)
            rhs = jnp.concatenate([hh[:, cols], hl[:, cols], hh[:, cols]], axis=0)
            r = dot(lhs, rhs)
            for j in range(2):
                n = 2 * k + j
                scale = lax.rsqrt(column + sz[pl.ds(n, 1), :])
                last[i, :, 128 * n : 128 * n + 128] = r[:, 128 * j : 128 * j + 128] * scale
        pltpu.make_async_copy(last.at[i], out.at[c], out_sem).start()
    pltpu.make_async_copy(out, out, out_sem).wait()


def body(source, symbol_x, symbol_y, symbol_z):
    high, low = halves(table())
    order = np.array([a * 16 + c for c in range(EARLY) for a in range(32)])
    stacked = np.concatenate([high[order], low[order]])
    any_space = pl.BlockSpec(memory_space=pl.ANY)
    f32, bf16 = jnp.float32, jnp.bfloat16
    done, b_in, hh, hl = pl.pallas_call(
        kernel,
        out_shape=(
            pltpu.VMEM((16, 128, 512), f32),
            pltpu.VMEM((64, 128, 128), f32),
            pltpu.VMEM((512, 512), bf16),
            pltpu.VMEM((512, 512), bf16),
        ),
        in_specs=[any_space] * 7,
        out_specs=(pl.BlockSpec(memory_space=pltpu.VMEM),) * 4,
        scratch_shapes=[
            pltpu.VMEM((16, 512, 128), f32),
            pltpu.VMEM((16, 512, 128), bf16),
            pltpu.VMEM((16, 512, 128), bf16),
            pltpu.VMEM(stacked.shape, bf16),
            pltpu.VMEM((len(order) * 16, 128), f32),
            pltpu.VMEM((8192, 128), f32),
            pltpu.VMEM((8192, 128), f32),
            pltpu.VMEM((64, 128, 128), f32),
            pltpu.VMEM((128, 128), f32),
            pltpu.SMEM((512,), f32),
            pltpu.VMEM((4, 128), f32),
            pltpu.VMEM((4, 128), f32),
            pltpu.SemaphoreType.DMA((len(GROUPS),)),
            pltpu.SemaphoreType.DMA((6,)),
            pltpu.SemaphoreType.DMA,
            pltpu.SemaphoreType.DMA((16,)),
            pltpu.SemaphoreType.DMA,
            pltpu.SemaphoreType.DMA((16,)),
        ],
        compiler_params=pltpu.CompilerParams(
            collective_id=0, has_side_effects=True, vmem_limit_bytes=67043328 - 9 * 1024 * 1024 - 65536
        ),
    )(
        source.reshape(512, 16, 1, 128),
        jnp.asarray(stacked),
        jnp.asarray(high),
        jnp.asarray(low),
        symbol_x,
        symbol_y.reshape(4, 128),
        symbol_z.reshape(4, 128),
    )
    return pl.pallas_call(
        finish,
        out_shape=jax.ShapeDtypeStruct((16, 128, 512), f32),
        in_specs=[pl.BlockSpec(memory_space=pltpu.VMEM)] * 4 + [any_space] * 3,
        out_specs=any_space,
        scratch_shapes=[
            pltpu.VMEM((FINAL, 128, 512), f32),
            pltpu.SMEM((512,), f32),
            pltpu.VMEM((4, 128), f32),
            pltpu.VMEM((4, 128), f32),
            pltpu.SemaphoreType.DMA,
            pltpu.SemaphoreType.DMA((3,)),
        ],
        compiler_params=pltpu.CompilerParams(vmem_limit_bytes=32 * 1024 * 1024),
    )(done, b_in, hh, hl, symbol_x, symbol_y.reshape(4, 128), symbol_z.reshape(4, 128))


def solution(mesh):
    placed = (P(None, "ya", "zb"), P(), P(), P())
    return jax.shard_map(
        body, mesh=mesh, in_specs=placed, out_specs=P("ya", "zb", None), check_vma=False
    )
```

```python
import functools

import jax
import jax.numpy as jnp
import ml_dtypes
import numpy as np
from jax import lax
from jax.experimental import pallas as pl
from jax.experimental.pallas import tpu as pltpu
from jax.sharding import PartitionSpec as P

MESH = pl.DeviceIdType.MESH


def scoped(f):
    def g(*args):
        with jax.named_scope(f.__name__):
            return f(*args)

    return g

N = 512
FAR = (10, 11, 14, 9, 6, 5, 7, 13, 15, 8, 2, 1, 4, 3, 12)
EARLY = 2
YPARTS = ((1, 3), (2, 0))
AHEAD = 3
LAG = 2
FINAL = 1
GROUPS = ((0, 4), (4, 4), (8, 4), (12, 4))


def table():
    rank = np.arange(1, N + 1)
    angle = np.pi * (rank[:, None] * rank[None, :] % (2 * N + 2)) / (N + 1)
    return np.sqrt(2.0 / (N + 1)) * np.sin(angle)


def halves(h):
    high = h.astype(ml_dtypes.bfloat16)
    return high, (h - high.astype(np.float64)).astype(ml_dtypes.bfloat16)


def split(v):
    high = v.astype(jnp.bfloat16)
    return high, (v - high.astype(jnp.float32)).astype(jnp.bfloat16)


def dot(a, b):
    return jnp.dot(a, b, preferred_element_type=jnp.float32)


def kernel(
    src, h1_hbm, hh_hbm, hl_hbm, sx_hbm, sy_hbm, sz_hbm, out, b_in, hh, hl,
    xin, xh, xl, h1, a_early, a_out, a_in, b_out, ycol, sx, sy, sz,
    load_sem, table_sem, a_send, a_recv, b_send, b_recv,
):
    ya, zb = lax.axis_index("ya"), lax.axis_index("zb")

    def load(y):
        group = max(g for g in range(len(GROUPS)) if GROUPS[g][0] <= y)
        return pltpu.make_async_copy(src.at[:, y, 0, :], xin.at[y], load_sem.at[group])

    tables = [
        pltpu.make_async_copy(s, d, table_sem.at[k])
        for k, (s, d) in enumerate(
            ((h1_hbm, h1), (hh_hbm, hh), (hl_hbm, hl), (sx_hbm, sx), (sy_hbm, sy), (sz_hbm, sz))
        )
    ]
    tables[0].start()
    for y in range(4):
        load(y).start()

    z0, y0 = ya >> 3, (ya >> 1) & 3
    peers = [z * 8 + y * 2 + k for k in (1, 0) for z in (0, 1, 3, 2) for y in (0, 1, 3, 2)]

    barrier = pltpu.get_barrier_semaphore()
    for peer in peers:

        @pl.when(peer != ya)
        def _():
            pl.semaphore_signal(barrier, inc=1, device_id=(peer, zb), device_id_type=MESH)

    for d in (1, 3, 2):
        pl.semaphore_signal(barrier, inc=1, device_id=(ya, (zb + d) & 3), device_id_type=MESH)
    for y in range(4, 16):
        load(y).start()

    def a_slot(c, who):
        return a_in.at[pl.ds(pl.multiple_of(c * 512 + who * 16, 16), 16)]

    def a_source(c, who):
        if isinstance(c, int) and c < EARLY:
            return a_early.at[pl.ds(pl.multiple_of(c * 512 + who * 16, 16), 16)]
        return a_out.at[pl.ds(pl.multiple_of(who * 256 + c * 16, 16), 16)]

    @scoped
    def send_a(c):
        pltpu.make_async_copy(a_source(c, ya), a_slot(c, ya), a_recv.at[c % 8]).start()
        for peer in peers:

            @pl.when(peer != ya)
            def _():
                pltpu.make_async_remote_copy(
                    src_ref=a_source(c, peer),
                    dst_ref=a_slot(c, ya),
                    send_sem=a_send,
                    recv_sem=a_recv.at[c % 8],
                    device_id=(peer, zb),
                    device_id_type=MESH,
                ).start()

    @scoped
    def wait_a(c):
        slots = a_in.at[pl.ds(pl.multiple_of(c * 512, 512), 512)]
        pltpu.make_async_copy(slots, slots, a_recv.at[c % 8]).wait()

    @scoped
    def transform_y(c):
        bh, bl = split(a_in[pl.ds(pl.multiple_of(c * 512, 512), 512), :])
        rhs = jnp.concatenate([bh, bh, bl], axis=0)
        for blocks in ((0, 1), (3, 2)):
            rows = [slice(128 * b, 128 * b + 128) for b in blocks]
            high = jnp.concatenate([hh[r, :] for r in rows], axis=0)
            low = jnp.concatenate([hl[r, :] for r in rows], axis=0)
            r = dot(jnp.concatenate([high, low, high], axis=1), rhs)
            for i, b in enumerate(blocks):
                b_out[c * 4 + b] = r[128 * i : 128 * i + 128, :]

                @pl.when(zb != b)
                def _():
                    pltpu.make_async_remote_copy(
                        src_ref=b_out.at[c * 4 + b],
                        dst_ref=b_in.at[c * 4 + zb],
                        send_sem=b_send,
                        recv_sem=b_recv.at[c % 8],
                        device_id=(ya, b),
                        device_id_type=MESH,
                    ).start()

                @pl.when(zb == b)
                def _():
                    pltpu.make_async_copy(b_out.at[c * 4 + b], b_in.at[c * 4 + b], b_recv.at[c % 8]).start()

    @scoped
    def wait_b(c):
        slots = b_in.at[pl.ds(c * 4, 4)]
        pltpu.make_async_copy(slots, slots, b_recv.at[c % 8]).wait()

    @scoped
    def transform_z(c):
        ah, al = split(jnp.concatenate([b_in[c * 4 + b] for b in range(4)], axis=1))
        lhs = jnp.concatenate([ah, ah, al], axis=1)
        column = ycol[...] + sx[ya * 16 + c]
        for k in range(2):
            cols = slice(256 * k, 256 * k + 256)
            rhs = jnp.concatenate([hh[:, cols], hl[:, cols], hh[:, cols]], axis=0)
            r = dot(lhs, rhs)
            for j in range(2):
                n = 2 * k + j
                scale = lax.rsqrt(column + sz[pl.ds(n, 1), :])
                out[c, :, 128 * n : 128 * n + 128] = r[:, 128 * j : 128 * j + 128] * scale

    rows = 32 * EARLY
    with jax.named_scope("early"):
        for g, (y0, ny) in enumerate(GROUPS):
            bhs, bls = [], []
            landed = xin.at[pl.ds(y0, ny)]
            with jax.named_scope(f"ld{g}"):
                pltpu.make_async_copy(landed, landed, load_sem.at[g]).wait()
            for y in range(y0, y0 + ny):
                high, low = split(xin[y])
                xh[y] = high
                xl[y] = low
                bhs.append(high)
                bls.append(low)
            if g == 2:
                for t in tables[1:]:
                    t.start()
            if g == 0:
                with jax.named_scope("tab"):
                    tables[0].wait()
            bh, bl = jnp.concatenate(bhs, axis=1), jnp.concatenate(bls, axis=1)
            both = dot(h1[...], bh)
            r = both[:rows] + (both[rows:] + dot(h1[pl.ds(0, rows), :], bl))
            for k in range(ny):
                a_early[pl.ds(y0 + k, rows, stride=16), :] = r[:, 128 * k : 128 * k + 128]
    with jax.named_scope("barrier_wait"):
        pl.semaphore_wait(barrier, 34)
    send_a(0)
    for t in tables[1:]:
        t.wait()
    with jax.named_scope("rest"):

        @pl.loop(0, 2, unroll=2)
        def _(g):
            bh = jnp.concatenate([xh[2 * g + k] for k in range(2)], axis=1)
            bl = jnp.concatenate([xl[2 * g + k] for k in range(2)], axis=1)
            rhs = jnp.concatenate([bh, bh, bl], axis=0)
            for p in range(1):
                rows = slice(512 * p, 512 * p + 512)
                r = dot(jnp.concatenate([hh[rows, :], hl[rows, :], hh[rows, :]], axis=1), rhs)
                for k in range(2):
                    a_out[pl.ds(512 * 16 * p + 2 * g + k, 512, stride=16), :] = r[:, 128 * k : 128 * k + 128]

        send_a(1)

        @pl.loop(2, 8, unroll=3)
        def _(g):
            bh = jnp.concatenate([xh[2 * g + k] for k in range(2)], axis=1)
            bl = jnp.concatenate([xl[2 * g + k] for k in range(2)], axis=1)
            rhs = jnp.concatenate([bh, bh, bl], axis=0)
            for p in range(1):
                rows = slice(512 * p, 512 * p + 512)
                r = dot(jnp.concatenate([hh[rows, :], hl[rows, :], hh[rows, :]], axis=1), rhs)
                for k in range(2):
                    a_out[pl.ds(512 * 16 * p + 2 * g + k, 512, stride=16), :] = r[:, 128 * k : 128 * k + 128]

    @pl.loop(EARLY, AHEAD)
    def _(c):
        send_a(c)

    ycol[...] = jnp.transpose(jnp.broadcast_to(sy[pl.ds(zb, 1), :], (128, 128)))

    @pl.loop(0, 16)
    def _(c):
        wait_a(c)
        transform_y(c)

        @pl.when(c + AHEAD < 16)
        def _():
            send_a(c + AHEAD)

        @pl.when(c >= LAG)
        def _():
            wait_b(c - LAG)
            transform_z(c - LAG)

    @pl.loop(16 - LAG, 16)
    def _(c):
        wait_b(c)

        @pl.when(c < 15)
        def _():
            transform_z(c)

    with jax.named_scope("drain"):

        sent = a_in.at[pl.ds(0, 16 * 31 * 16)]
        pltpu.make_async_copy(sent, sent, a_send).wait()
        sent = b_out.at[pl.ds(0, 16 * 3)]
        pltpu.make_async_copy(sent, sent, b_send).wait()


def finish(done, b_in, hh, hl, sx_hbm, sy_hbm, sz_hbm, out, last, sx, sy, sz, out_sem, sem):
    ya, zb = lax.axis_index("ya"), lax.axis_index("zb")
    loads = [pltpu.make_async_copy(s, d, sem.at[k]) for k, (s, d) in enumerate(((sx_hbm, sx), (sy_hbm, sy), (sz_hbm, sz)))]
    for t in loads:
        t.start()
    first = 16 - FINAL
    for k in range(5):
        pltpu.make_async_copy(done.at[pl.ds(3 * k, 3)], out.at[pl.ds(3 * k, 3)], out_sem).start()
    for t in loads:
        t.wait()
    ycol = jnp.transpose(jnp.broadcast_to(sy[pl.ds(zb, 1), :], (128, 128)))
    for i in range(FINAL):
        c = first + i
        ah, al = split(jnp.concatenate([b_in[c * 4 + b] for b in range(4)], axis=1))
        lhs = jnp.concatenate([ah, ah, al], axis=1)
        column = ycol + sx[ya * 16 + c]
        for k in range(2):
            cols = slice(256 * k, 256 * k + 256)
            rhs = jnp.concatenate([hh[:, cols], hl[:, cols], hh[:, cols]], axis=0)
            r = dot(lhs, rhs)
            for j in range(2):
                n = 2 * k + j
                scale = lax.rsqrt(column + sz[pl.ds(n, 1), :])
                last[i, :, 128 * n : 128 * n + 128] = r[:, 128 * j : 128 * j + 128] * scale
        pltpu.make_async_copy(last.at[i], out.at[c], out_sem).start()
    pltpu.make_async_copy(out, out, out_sem).wait()


def body(source, symbol_x, symbol_y, symbol_z):
    high, low = halves(table())
    order = np.array([a * 16 + c for c in range(EARLY) for a in range(32)])
    stacked = np.concatenate([high[order], low[order]])
    any_space = pl.BlockSpec(memory_space=pl.ANY)
    f32, bf16 = jnp.float32, jnp.bfloat16
    done, b_in, hh, hl = pl.pallas_call(
        kernel,
        out_shape=(
            pltpu.VMEM((16, 128, 512), f32),
            pltpu.VMEM((64, 128, 128), f32),
            pltpu.VMEM((512, 512), bf16),
            pltpu.VMEM((512, 512), bf16),
        ),
        in_specs=[any_space] * 7,
        out_specs=(pl.BlockSpec(memory_space=pltpu.VMEM),) * 4,
        scratch_shapes=[
            pltpu.VMEM((16, 512, 128), f32),
            pltpu.VMEM((16, 512, 128), bf16),
            pltpu.VMEM((16, 512, 128), bf16),
            pltpu.VMEM(stacked.shape, bf16),
            pltpu.VMEM((len(order) * 16, 128), f32),
            pltpu.VMEM((8192, 128), f32),
            pltpu.VMEM((8192, 128), f32),
            pltpu.VMEM((64, 128, 128), f32),
            pltpu.VMEM((128, 128), f32),
            pltpu.SMEM((512,), f32),
            pltpu.VMEM((4, 128), f32),
            pltpu.VMEM((4, 128), f32),
            pltpu.SemaphoreType.DMA((len(GROUPS),)),
            pltpu.SemaphoreType.DMA((6,)),
            pltpu.SemaphoreType.DMA,
            pltpu.SemaphoreType.DMA((8,)),
            pltpu.SemaphoreType.DMA,
            pltpu.SemaphoreType.DMA((8,)),
        ],
        compiler_params=pltpu.CompilerParams(
            collective_id=0, has_side_effects=True, vmem_limit_bytes=67043328 - 9 * 1024 * 1024 - 65536
        ),
    )(
        source.reshape(512, 16, 1, 128),
        jnp.asarray(stacked),
        jnp.asarray(high),
        jnp.asarray(low),
        symbol_x,
        symbol_y.reshape(4, 128),
        symbol_z.reshape(4, 128),
    )
    return pl.pallas_call(
        finish,
        out_shape=jax.ShapeDtypeStruct((16, 128, 512), f32),
        in_specs=[pl.BlockSpec(memory_space=pltpu.VMEM)] * 4 + [any_space] * 3,
        out_specs=any_space,
        scratch_shapes=[
            pltpu.VMEM((FINAL, 128, 512), f32),
            pltpu.SMEM((512,), f32),
            pltpu.VMEM((4, 128), f32),
            pltpu.VMEM((4, 128), f32),
            pltpu.SemaphoreType.DMA,
            pltpu.SemaphoreType.DMA((3,)),
        ],
        compiler_params=pltpu.CompilerParams(vmem_limit_bytes=32 * 1024 * 1024),
    )(done, b_in, hh, hl, symbol_x, symbol_y.reshape(4, 128), symbol_z.reshape(4, 128))


def solution(mesh):
    placed = (P(None, "ya", "zb"), P(), P(), P())
    return jax.shard_map(
        body, mesh=mesh, in_specs=placed, out_specs=P("ya", "zb", None), check_vma=False
    )
```
